256 devices in a mesh: mrow: 8 (over y, z_lo), pcol: 32 (over x, z_hi, core).
Axes of the slice: x: 4, y: 4, z: 8 (z_hi: 4, z_lo: 2; z = z_hi * 2 + z_lo), core: 2. Of those that a mesh axis runs over, the one named last changes fastest.
Arguments:
- snapshots: bfloat16 [7424, 8192], P('mrow', 'pcol'), may hold values from -16 to 16
- area_weight: float32 [8192], P('pcol'), may hold values from 0.2 to 1
Outputs:
- gram_tiles: float32 [8, 32, 215296], P('mrow', 'pcol')
The draws below stay inside these ranges and needn't reach their ends.
All inputs are finite; a program needn't handle non-finite values.
Results may differ from the reference program's by a relative error of at most 0.0003.
Values may be sent and summed in bfloat16 or wider, within the bound.
No kernel may reach another device: no remote copies, remote signals or barrier semaphores. Data moves between devices by JAX's collectives and lax.ppermute only.
A program may use at most 64 MiB of HBM per device.

```python
import math
import jax
import jax.numpy as jnp
from jax import lax

MEMBERS = 7424
POINTS = 8192
N_MROW = 8
N_PCOL = 32


def draw_snapshots(key, part):
    base = jax.random.fold_in(key, 11)
    keys = jax.random.split(base, 6)
    mode_count = 96
    climate = 2.0 * jax.random.normal(keys[0], (1, POINTS), jnp.float32)
    ranks = jnp.arange(1, mode_count + 1).astype(jnp.float32)
    coeff = jax.random.normal(keys[1], (MEMBERS, mode_count), jnp.float32) * (ranks ** (-0.5))[None, :]
    freq = jax.random.randint(keys[2], (mode_count, 1), 1, 33).astype(jnp.float32)
    phase = jax.random.uniform(keys[3], (mode_count, 1), jnp.float32, 0.0, 2.0 * math.pi)
    position = (jnp.arange(POINTS).astype(jnp.float32) / POINTS)[None, :]
    shapes = math.sqrt(2.0) * jnp.cos(2.0 * math.pi * freq * position + phase)
    rough = jax.random.uniform(keys[4], (1, POINTS), jnp.float32, 0.6, 1.4)
    total_var = jnp.sum(1.0 / ranks)
    signal = jnp.dot(coeff, shapes, precision=lax.Precision.HIGHEST) / jnp.sqrt(total_var) * rough
    noise = jax.random.normal(keys[5], (MEMBERS, POINTS), jnp.float32)
    field = signal + 0.2 * noise
    return jnp.clip(climate + field, -16.0, 16.0).astype(jnp.bfloat16)


def levels(own_key, shape, cuts, low, top_value):
    loudness = 1.0
    for dim, shards_of in cuts:
        draws = jax.random.uniform(jax.random.fold_in(jax.random.fold_in(own_key, 6), dim), (shards_of,), jnp.float32, low / len(cuts), top_value / len(cuts))
        loudness = loudness * jnp.repeat(jnp.exp(draws), shape[dim] // shards_of).reshape((-1,) + (1,) * (len(shape) - 1 - dim))
    return loudness


def setup_inputs(seed: int = 0) -> dict:
    key_list = jax.random.split(jax.random.key(seed), 3)
    snapshots = draw_snapshots(jax.random.fold_in(key_list[2], 71), 0)
    area_weight = jnp.clip(jnp.exp(math.log(1.0) - 1.609438 * jax.random.uniform(key_list[1], (POINTS,), jnp.float32) ** levels(key_list[1], (POINTS,), ((0, 32),), -0.2, 0.2)), 0.2, 1.0)
    return {"snapshots": snapshots, "area_weight": area_weight}


def reference(snapshots, area_weight):
    ens_mean = lax.optimization_barrier(jnp.sum(snapshots.astype(jnp.float32), axis=0)) / MEMBERS
    anomaly = ((snapshots.astype(jnp.float32) - ens_mean[None, :]) * jnp.sqrt(area_weight)[None, :]).astype(jnp.bfloat16)
    wide = anomaly.astype(jnp.float32)
    gram = jnp.dot(wide, wide.T, precision=lax.Precision.HIGHEST, preferred_element_type=jnp.float32)
    gram = gram / (MEMBERS - 1)
    blocks = gram.reshape(N_MROW, MEMBERS // N_MROW, N_PCOL, MEMBERS // N_PCOL)
    blocks = jnp.transpose(blocks, (0, 2, 1, 3))
    return blocks.reshape(N_MROW, N_PCOL, MEMBERS // N_MROW * (MEMBERS // N_PCOL))
```

```python
import jax
import jax.numpy as jnp
from jax import lax
from jax.experimental import pallas as pl
from jax.experimental.pallas import tpu as pltpu
from jax.sharding import Mesh
from jax.sharding import PartitionSpec as P

MEMBERS = 7424
AXES = ("y", "zl", "x", "zh", "c")
ROWS = ("y", "zl")
COLS = ("x", "zh", "c")


def shift(value, axis, by):
    n = lax.axis_size(axis)
    return lax.ppermute(value, axis, [(i, (i + by) % n) for i in range(n)])


def swap(value, axis):
    return lax.ppermute(value, axis, [(0, 1), (1, 0)])


def sent_to_all(value, axes):
    copies = jnp.broadcast_to(value, (lax.axis_size(axes), *value.shape))
    return lax.all_to_all(copies, axes, split_axis=0, concat_axis=0, tiled=True)


def transposed(block, k):
    pairs = []
    for y in range(4):
        for zl in range(2):
            for x in range(4):
                for zh in range(4):
                    a, b = zh // 2, zh % 2
                    source = ((y * 2 + zl) * 4 + x) * 4 + zh
                    target = ((x * 2 + a) * 4 + y) * 4 + 2 * zl + (k ^ b)
                    pairs.append((source, target))
    return lax.ppermute(block, ("y", "zl", "x", "zh"), pairs)


def ring(value, axis, half):
    behind = shift(value, axis, 1)
    ahead = shift(value, axis, -1)
    far_a = shift(behind[:half], axis, 1)
    far_b = shift(ahead[half:], axis, -1)
    return value, behind, ahead, far_a, far_b


def gram_kernel(index, stats, *refs):
    half = refs[0].shape[0] // 2
    tile = half // 2
    row_refs, col_refs = refs[:20], refs[20:30]
    out, cols = refs[30], refs[31]

    def anomaly(value, where):
        wide = value.astype(jnp.float32) - stats[where, 0:1, :]
        return wide * stats[where, 1:2, :]

    def put(value, where):
        wide = anomaly(value, where)
        cols[where * 2] = wide[:tile].astype(jnp.bfloat16)
        cols[where * 2 + 1] = wide[tile:].astype(jnp.bfloat16)

    core = index[32]
    for g in range(2):
        own, behind, ahead, far_a, far_b = col_refs[5 * g : 5 * g + 5]
        for k in range(2):
            at = 16 + g * 8 + k
            put(own[k * half : (k + 1) * half], index[at])
            put(behind[k * half : (k + 1) * half], index[at + 2])
            put(ahead[k * half : (k + 1) * half], index[at + 4])
            put((far_a, far_b)[k][...], index[at + 6])

    contract = (((1,), (1,)), ((), ()))
    out[...] = jnp.zeros_like(out)

    def add(value, where, rows):
        left = anomaly(value, where).astype(jnp.bfloat16)
        for slot in range(2):
            out[slot, rows] += lax.dot_general(
                left,
                cols[where * 2 + lax.rem(core + slot, 2)],
                contract,
                preferred_element_type=jnp.float32,
            )

    for g in range(4):
        own, behind, ahead, far_a, far_b = row_refs[5 * g : 5 * g + 5]
        at = g * 4
        add(own[...], index[at], pl.ds(0, 2 * half))
        add(behind[...], index[at + 1], pl.ds(0, 2 * half))
        add(ahead[...], index[at + 2], pl.ds(0, 2 * half))
        add(far_a[...], index[at + 3], pl.ds(0, half))
        add(far_b[...], index[at + 3], pl.ds(half, half))


def local(snapshots, area_weight):
    rows, points = snapshots.shape
    half = rows // 2
    y, zl, x, zh, c = (lax.axis_index(a) for a in AXES)

    row_parts = list(ring(snapshots, "x", half))
    _, z_behind, z_ahead, z_far_a, z_far_b = ring(snapshots, "zh", half)
    bit = zh % 2
    t0 = transposed(lax.dynamic_slice_in_dim(snapshots, bit * half, half, 0), 0)
    t1 = transposed(lax.dynamic_slice_in_dim(snapshots, (1 - bit) * half, half, 0), 1)
    turned = jnp.concatenate([t0, t1], axis=0)
    col_parts = list(ring(turned, "y", half))
    other = swap(turned, "zl")
    row_parts += ring(z_behind, "x", half)
    row_parts += ring(z_ahead, "x", half)
    col_parts += ring(other, "y", half)
    row_parts += ring(jnp.concatenate([z_far_a, z_far_b], axis=0), "x", half)

    local_sum = jnp.sum(snapshots.astype(jnp.float32), axis=0)
    ens_mean = jnp.sum(sent_to_all(local_sum, ROWS), axis=0) / MEMBERS
    stats = jnp.stack([ens_mean, jnp.sqrt(area_weight)])
    stats = sent_to_all(stats, ("x", "zh"))

    index = []
    for dz in (0, -1, 1, 2):
        for dx in (0, -1, 1, 2):
            index.append((x + dx + 4) % 4 * 4 + (zh + dz + 4) % 4)
    for g in range(2):
        a = (zl + g) % 2
        for dy in (0, -1, 1, 2):
            for k in range(2):
                index.append((y + dy + 4) % 4 * 4 + 2 * a + (k + zh) % 2)
    index.append(c)
    index = jnp.stack(index).astype(jnp.int32)

    vmem = pl.BlockSpec(memory_space=pltpu.VMEM)
    partial = pl.pallas_call(
        gram_kernel,
        out_shape=jax.ShapeDtypeStruct((2, rows, half // 2), jnp.float32),
        in_specs=[pl.BlockSpec(memory_space=pltpu.SMEM)] + [vmem] * 31,
        out_specs=vmem,
        scratch_shapes=[pltpu.VMEM((32, half // 2, points), jnp.bfloat16)],
        compiler_params=pltpu.CompilerParams(vmem_limit_bytes=48 * 2**20),
        name="gram",
    )(index, stats, *row_parts, *col_parts)
    gram = (partial[0] + swap(partial[1], "c")) / (MEMBERS - 1)
    return gram.reshape(1, 1, -1)


def solution(mesh):
    torus = Mesh(mesh.devices.reshape(4, 2, 4, 4, 2), AXES)
    return jax.shard_map(
        local,
        mesh=torus,
        in_specs=(P(ROWS, COLS), P(COLS)),
        out_specs=P(ROWS, COLS, None),
        check_vma=False,
    )
```
